32 devices in a mesh: vocab: 16 (over z, y, x), width: 2 (over core).
Axes of the slice: x: 2, y: 2, z: 4, core: 2. Of those that a mesh axis runs over, the one named last changes fastest.
Arguments:
- token_grads: bfloat16 [16384, 4608], P('vocab', 'width'), may hold values from -6 to 6
- token_slot: int32 [16384], P('vocab'), may hold values from 0 to 255, as said below
- slot_rows: int32 [16, 256], P('vocab'), may hold values from 0 to 1023, as said below
- counts: int32 [16, 16], P('vocab'), may hold values from 1 to 16, as said below
- weights: bfloat16 [16384, 4608], P('vocab', 'width'), may hold values from -0.29882812 to 0.29882812
- moment: bfloat16 [16384, 4608], P('vocab', 'width'), may hold values from -2 to 2
- row_scale: float32 [16384], P('vocab'), may hold values from 0.1 to 4
- row_steps: int32 [16384], P('vocab'), may hold values from 0 to 11
Outputs:
- new_weights: bfloat16 [16384, 4608], P('vocab', 'width')
- new_moment: bfloat16 [16384, 4608], P('vocab', 'width')
- new_scale: float32 [16384], P('vocab')
The draws below stay inside these ranges and needn't reach their ends.
Inputs may be any that keep to these rules, and one draw needn't show every extreme that they name: `token_slot`: each token names a live slot of its own source. `slot_rows`: within one source and one owner the 16 entries are distinct. `counts`: in every draw some owners receive 16 live slots from every source.
All inputs are finite; a program needn't handle non-finite values.
Results may differ from the reference program's by a relative error of at most 0.0011.
Values may be sent and summed in bfloat16 or wider, within the bound.
No kernel may reach another device: no remote copies, remote signals or barrier semaphores. Data moves between devices by JAX's collectives and lax.ppermute only.
A program may use at most 128 MiB of HBM per device.

```python
import math
import jax
import jax.numpy as jnp
from jax import lax

D = 4608
VOC_DEV = 1024
CAP = 16
TOK_DEV = 1024
OWNERS = 16
TOKENS = 16384
VOCAB = 16384


def routing(key):
    base = jax.random.fold_in(key, 7)
    key_hot, key_small, key_rows, key_pick = jax.random.split(base, 4)
    hot = jax.random.permutation(key_hot, OWNERS) < max(OWNERS // 8, 1)
    small = jax.random.randint(key_small, (OWNERS, OWNERS), 1, max(CAP // 4, 1) + 1)
    counts = jnp.where(hot[None, :], CAP, small).astype(jnp.int32)
    row_keys = jax.random.split(key_rows, OWNERS * OWNERS)
    picked = jax.vmap(lambda k: jax.random.permutation(k, VOC_DEV)[:CAP])(row_keys)
    slot_rows = picked.reshape(OWNERS, OWNERS * CAP).astype(jnp.int32)
    within = jnp.arange(CAP, dtype=jnp.int32)
    live = (within[None, None, :] < counts[:, :, None]).reshape(OWNERS, OWNERS * CAP)
    order_key = jnp.where(live, 0, 1) * (OWNERS * CAP) + jnp.arange(OWNERS * CAP, dtype=jnp.int32)[None, :]
    order = jnp.argsort(order_key, axis=1, stable=True).astype(jnp.int32)
    live_count = jnp.sum(live.astype(jnp.int32), axis=1)
    raw = jax.random.randint(key_pick, (OWNERS, TOK_DEV), 0, 1 << 30)
    pick = raw % live_count[:, None]
    token_slot = jnp.take_along_axis(order, pick, axis=1).reshape(TOKENS).astype(jnp.int32)
    return (token_slot, slot_rows, counts)


def draw_token_slot(key, part):
    return routing(key)[0]


def draw_slot_rows(key, part):
    return routing(key)[1]


def draw_counts(key, part):
    return routing(key)[2]


def set_ends(values, key, smallest, largest):
    dims = values.shape
    place = [jax.random.randint(jax.random.fold_in(key, axis), (), 0, dims[axis]) for axis in range(len(dims))]
    values = values.at[tuple(place)].set(smallest)
    longest = dims.index(max(dims))
    place[longest] = (place[longest] + 1) % dims[longest]
    return values.at[tuple(place)].set(largest)


def levels(stream_key, shape, cuts, least, largest):
    factor_of, own = 1.0, jax.random.fold_in(stream_key, 6)
    for axis_at, parts in cuts:
        draws = jnp.exp(jax.random.uniform(jax.random.fold_in(own, axis_at), (parts,), jnp.float32, least / len(cuts), largest / len(cuts)))
        factor_of = factor_of * jnp.repeat(draws, shape[axis_at] // parts).reshape([-1 if axis == axis_at else 1 for axis in range(len(shape))])
    return factor_of


def scatter_about(own_key, shape, deviation, limit, cuts=(), kind=jnp.bfloat16):
    level = levels(own_key, shape, cuts, -0.22, 0.18) if cuts else 1.0
    entries = jax.random.normal(own_key, shape, jnp.float32) * deviation * level
    return jnp.minimum(jnp.maximum(entries, -limit), limit).astype(kind)


def setup_inputs(seed: int = 0) -> dict:
    streams_of = jax.random.split(jax.random.key(seed), 9)
    token_grads = scatter_about(streams_of[0], (TOKENS, D), 1.0, 6.0, ((0, 16), (1, 2)))
    token_slot = draw_token_slot(jax.random.fold_in(streams_of[8], 71), 0)
    slot_rows = draw_slot_rows(jax.random.fold_in(streams_of[8], 71), 0)
    counts = draw_counts(jax.random.fold_in(streams_of[8], 71), 0)
    weights = scatter_about(streams_of[4], (VOCAB, D), 0.05, 0.29882812, ((0, 16), (1, 2)))
    moment = scatter_about(streams_of[5], (VOCAB, D), 0.3, 2.0, ((0, 16), (1, 2)))
    row_scale = jnp.clip(jnp.exp(math.log(4.0) - 3.6888794 * jax.random.uniform(streams_of[6], (VOCAB,), jnp.float32) ** levels(streams_of[6], (VOCAB,), ((0, 16),), -0.2, 0.2)), 0.1, 4.0)
    row_steps = set_ends(jax.random.randint(streams_of[7], (VOCAB,), 0, 12), jax.random.fold_in(streams_of[7], 1), 0, 11).astype(jnp.int32)
    return {"token_grads": token_grads, "token_slot": token_slot, "slot_rows": slot_rows, "counts": counts, "weights": weights, "moment": moment, "row_scale": row_scale, "row_steps": row_steps}


def reference(token_grads, token_slot, slot_rows, counts, weights, moment, row_scale, row_steps):
    slots_all = OWNERS * CAP
    source = jnp.arange(TOKENS, dtype=jnp.int32) // TOK_DEV
    segment = source * slots_all + token_slot
    slot_grads = jax.ops.segment_sum(token_grads.astype(jnp.float32), segment, num_segments=OWNERS * slots_all).astype(jnp.bfloat16)
    position = jnp.arange(slots_all, dtype=jnp.int32)
    owner = position // CAP
    within = position % CAP
    live = within[None, :] < jnp.take_along_axis(counts, jnp.broadcast_to(owner[None, :], (OWNERS, slots_all)), axis=1)
    target = jnp.where(live, owner[None, :] * VOC_DEV + slot_rows, VOCAB).reshape(-1)
    grad = jax.ops.segment_sum(slot_grads.astype(jnp.float32), target, num_segments=VOCAB + 1)[:VOCAB]
    hits = jax.ops.segment_sum(jnp.ones_like(target), target, num_segments=VOCAB + 1)[:VOCAB]
    touched = hits > 0
    square = lax.optimization_barrier(jnp.sum(grad * grad, axis=1)) / D
    step_count = (row_steps + 1).astype(jnp.float32)
    first = 0.9 * moment.astype(jnp.float32) + 0.1 * grad
    second = 0.95 * row_scale + 0.05 * square
    first = jnp.where(touched[:, None], first, moment.astype(jnp.float32))
    second = jnp.where(touched, second, row_scale)
    fix_first = 1.0 - jnp.power(jnp.float32(0.9), step_count)
    fix_second = 1.0 - jnp.power(jnp.float32(0.95), step_count)
    denom = jnp.sqrt(second / fix_second) + 1e-08
    old = weights.astype(jnp.float32)
    stepped = old - 0.01 * (first / fix_first[:, None] / denom[:, None] + 0.1 * old)
    new_weights = jnp.where(touched[:, None], stepped, old).astype(jnp.bfloat16)
    return (new_weights, first.astype(jnp.bfloat16), second)
```

```python
import functools

import jax
import jax.numpy as jnp
from jax import lax
from jax.experimental import pallas as pl
from jax.experimental.pallas import tpu as pltpu
from jax.sharding import PartitionSpec as P


LANES = 128
MIB = 1 << 20
VMEM = pl.BlockSpec(memory_space=pltpu.VMEM)
SMEM = pl.BlockSpec(memory_space=pltpu.SMEM)
ANY = pl.BlockSpec(memory_space=pl.ANY)
F32, BF16, I32 = jnp.float32, jnp.bfloat16, jnp.int32


def iota(shape, axis):
    return lax.broadcasted_iota(I32, shape, axis)


def name_rows(slots):
    return -(-2 * (slots // LANES) // 8) * 8


def col_step(half):
    return 2 * LANES if half % (2 * LANES) == 0 else LANES


def send_kernel(
    owners, cap, me_ref, counts_far, slot_far, rows_far, grads_ref, *rest
):
    outs, rest = rest[:owners], rest[owners:]
    onehot, buf, counts_ref, slot_ref, rows_ref, sems, small = rest
    tokens, half = grads_ref.shape
    slots = owners * cap
    step = col_step(half)
    copies = [
        pltpu.make_async_copy(
            grads_ref.at[:, pl.ds(c, step)], buf.at[:, pl.ds(c, step)], sems.at[c // step]
        )
        for c in range(0, half, step)
    ]
    arrivals = [
        pltpu.make_async_copy(far, ref, small.at[i])
        for i, (far, ref) in enumerate(
            ((slot_far, slot_ref), (rows_far, rows_ref), (counts_far, counts_ref))
        )
    ]
    for copy in arrivals + copies:
        copy.start()
    for copy in arrivals:
        copy.wait()
    me = me_ref[0]
    groups = slots // LANES
    turned = jnp.bitwise_xor(slot_ref[...], me * cap)
    for t in range(tokens // LANES):
        hit = turned[t : t + 1, :] == iota((slots, LANES), 0)
        onehot[:, t * LANES : (t + 1) * LANES] = jnp.where(hit, 1.0, 0.0).astype(BF16)
    lane = iota((1, slots), 1)
    owner, within = lane // cap, lax.rem(lane, cap)
    live = jnp.zeros((1, slots), I32)
    for o in range(owners):
        live = jnp.where((owner == o) & (within < counts_ref[0, o]), 1, live)
    rows = rows_ref[...]
    high = (rows // LANES + 1) * live
    low = lax.rem(rows, LANES) * live
    digits = jnp.concatenate(
        [high.astype(F32), low.astype(F32), jnp.zeros((6, slots), F32)], axis=0
    ).astype(BF16)
    turn = jnp.where(
        iota((slots, slots), 0) == jnp.bitwise_xor(iota((slots, slots), 1), me * cap), 1.0, 0.0
    ).astype(BF16)
    digits = jnp.dot(digits, turn, preferred_element_type=F32)
    pad = name_rows(slots) - 2 * groups
    names = [digits[0:1, g * LANES : (g + 1) * LANES] for g in range(groups)]
    names += [digits[1:2, g * LANES : (g + 1) * LANES] for g in range(groups)]
    if pad:
        names.append(jnp.zeros((pad, LANES), F32))
    names = jnp.concatenate(names, axis=0)
    base = half // LANES * cap
    sub, at = iota(names.shape, 0), iota(names.shape, 1)
    place = (lax.rem(sub, groups) * LANES + at) // cap
    for d in range(owners):
        outs[d][base:, :] = jnp.where(place == d, names, 0.0).astype(BF16)
    for c in range(0, half, step):
        copies[c // step].wait()
        got = jnp.dot(onehot[...], buf[:, c : c + step], preferred_element_type=F32).astype(BF16)
        for d in range(owners):
            for t in range(step // LANES):
                row = (c // LANES + t) * cap
                outs[d][row : row + cap, :] = got[
                    d * cap : (d + 1) * cap, t * LANES : (t + 1) * LANES
                ]


def grad_kernel(owners, cap, *refs):
    blocks = refs[:owners]
    grad_ref, squares_ref, hits_ref, count_ref, place, acc = refs[owners:]
    rows, half = grad_ref.shape
    slots = owners * cap
    groups = slots // LANES
    step = col_step(half)
    base = half // LANES * cap
    names = blocks[0][base:, :].astype(F32)
    for d in range(1, owners):
        names = names + blocks[d][base:, :].astype(F32)
    names = names.astype(I32)
    for g in range(groups):
        row = (names[g : g + 1, :] - 1) * LANES + names[groups + g : groups + g + 1, :]
        hit = row == iota((rows, LANES), 0)
        place[:, g * LANES : (g + 1) * LANES] = jnp.where(hit, 1.0, 0.0).astype(BF16)
    count_ref[...] = jnp.dot(
        place[...], jnp.ones((slots, LANES), BF16), preferred_element_type=F32
    )
    for c in range(0, half, step):
        parts = []
        for t in range(step // LANES):
            at = (c // LANES + t) * cap
            parts.append(jnp.concatenate([b[at : at + cap, :] for b in blocks], axis=0))
        got = jnp.concatenate(parts, axis=1) if len(parts) > 1 else parts[0]
        grad_ref[:, c : c + step] = jnp.dot(place[...], got, preferred_element_type=F32)
        for r in range(0, rows, LANES):
            total = acc[r : r + LANES, :] if c else None
            for t in range(step // LANES):
                x = grad_ref[r : r + LANES, c + t * LANES : c + (t + 1) * LANES]
                total = x * x if total is None else total + x * x
            acc[r : r + LANES, :] = total
    one = jnp.ones((8, LANES), F32)
    lanes = (((1,), (1,)), ((), ()))
    for r in range(rows // LANES):
        part = slice(r * LANES, (r + 1) * LANES)
        squares_ref[r : r + 1, :] = lax.dot_general(
            one, acc[part, :], lanes, precision=lax.Precision.HIGHEST, preferred_element_type=F32
        )[0:1, :]
        hits_ref[r : r + 1, :] = lax.dot_general(
            one, count_ref[part, :], lanes, precision=lax.Precision.HIGHEST, preferred_element_type=F32
        )[0:1, :]


def moment_kernel(grad_ref, count_ref, moment_ref, first_ref, new_ref, staged, sems):
    rows, half = grad_ref.shape
    strip = 16

    def copy(i):
        part = pl.ds(pl.multiple_of(i * LANES, LANES), LANES)
        return pltpu.make_async_copy(staged.at[part, :], new_ref.at[part, :], sems.at[i])

    @pl.loop(0, rows // LANES)
    def _(i):
        @pl.loop(0, LANES // strip)
        def _(j):
            part = pl.ds(pl.multiple_of(i * LANES + j * strip, strip), strip)
            keep = jnp.where(count_ref[part, :] > 0.0, 0.9, 1.0)
            for c in range(0, half, LANES):
                old = moment_ref[part, c : c + LANES].astype(F32)
                first = keep * old + 0.1 * grad_ref[part, c : c + LANES]
                first_ref[part, c : c + LANES] = first
                staged[part, c : c + LANES] = first.astype(BF16)

        copy(i).start()

    @pl.loop(0, rows // LANES)
    def _(i):
        copy(i).wait()


def weights_kernel(
    width, first_ref, weights_ref, mine_ref, other_ref, hits_ref, scale_ref, steps_ref,
    new_ref, new_scale_ref, staged, rates, sems,
):
    rows, half = first_ref.shape
    square = (mine_ref[...] + other_ref[...]) / width
    touched = hits_ref[...] > 0.5
    scale = scale_ref[...]
    second = jnp.where(touched, 0.95 * scale + 0.05 * square, scale)
    new_scale_ref[...] = second
    steps = (steps_ref[...] + 1).astype(F32)
    fix_first = 1.0 - jnp.exp(steps * jnp.log(jnp.float32(0.9)))
    fix_second = 1.0 - jnp.exp(steps * jnp.log(jnp.float32(0.95)))
    denom = jnp.sqrt(second / fix_second) + 1e-08
    rate = jnp.where(touched, 0.01 / (fix_first * denom), -1.0)
    eye = iota((LANES, LANES), 0) == iota((LANES, LANES), 1)
    for i in range(rows // LANES):
        column = jnp.sum(jnp.where(eye, rate[i : i + 1, :], 0.0), axis=1, keepdims=True)
        rates[i * LANES : (i + 1) * LANES, :] = jnp.broadcast_to(column, (LANES, LANES))
    strip = 16

    def copy(i):
        part = pl.ds(pl.multiple_of(i * LANES, LANES), LANES)
        return pltpu.make_async_copy(staged.at[part, :], new_ref.at[part, :], sems.at[i])

    @pl.loop(0, rows // LANES)
    def _(i):
        @pl.loop(0, LANES // strip)
        def _(j):
            part = pl.ds(pl.multiple_of(i * LANES + j * strip, strip), strip)
            rate = rates[part, :]
            keep = jnp.where(rate < 0.0, 1.0, 0.999)
            rate = jnp.maximum(rate, 0.0)
            for c in range(0, half, LANES):
                old = weights_ref[part, c : c + LANES].astype(F32)
                new = keep * old - rate * first_ref[part, c : c + LANES]
                staged[part, c : c + LANES] = new.astype(BF16)

        copy(i).start()

    @pl.loop(0, rows // LANES)
    def _(i):
        copy(i).wait()


def near(x):
    return pltpu.with_memory_space_constraint(x, pltpu.VMEM)


def far(x):
    return pltpu.with_memory_space_constraint(x, pltpu.HBM)


def params(limit):
    return pltpu.CompilerParams(vmem_limit_bytes=limit * MIB)


def shards(token_grads, token_slot, slot_rows, counts, weights, moment, row_scale, row_steps):
    owners = lax.axis_size("vocab")
    halves = lax.axis_size("width")
    slots = slot_rows.shape[1]
    cap = slots // owners
    tokens, half = token_grads.shape
    rows = weights.shape[0]
    assert owners & (owners - 1) == 0 and cap & (cap - 1) == 0
    assert rows % LANES == 0 and tokens % LANES == 0 and slots % LANES == 0 and half % LANES == 0
    me = lax.axis_index("vocab").astype(I32).reshape(1)
    height = half // LANES * cap + name_rows(slots)
    step = col_step(half)
    block = jax.ShapeDtypeStruct((height, LANES), BF16)
    outgoing = pl.pallas_call(
        functools.partial(send_kernel, owners, cap),
        out_shape=[block] * owners,
        in_specs=[SMEM, ANY, ANY, ANY, ANY],
        out_specs=[VMEM] * owners,
        scratch_shapes=[
            pltpu.VMEM((slots, tokens), BF16),
            pltpu.VMEM((tokens, half), BF16),
            pltpu.SMEM((1, owners), I32),
            pltpu.VMEM((tokens // LANES, LANES), I32),
            pltpu.VMEM((1, slots), I32),
            pltpu.SemaphoreType.DMA((half // step,)),
            pltpu.SemaphoreType.DMA((3,)),
        ],
        compiler_params=params(24),
        cost_estimate=pl.CostEstimate(
            flops=2 * slots * tokens * half, bytes_accessed=tokens * half * 2, transcendentals=0
        ),
        name="send",
    )(
        me, far(counts), far(token_slot.reshape(tokens // LANES, LANES)), far(slot_rows),
        far(token_grads),
    )
    received = {0: outgoing[0]}
    for d in range(1, owners):
        received[d] = lax.ppermute(outgoing[d], "vocab", [(s, s ^ d) for s in range(owners)])
    lined = jax.ShapeDtypeStruct((rows // LANES, LANES), F32)
    grad, squares, hits, count = pl.pallas_call(
        functools.partial(grad_kernel, owners, cap),
        out_shape=[pltpu.VMEM((rows, half), F32), lined, lined, pltpu.VMEM((rows, LANES), F32)],
        in_specs=[VMEM] * owners,
        out_specs=[VMEM] * 4,
        scratch_shapes=[pltpu.VMEM((rows, slots), BF16), pltpu.VMEM((rows, LANES), F32)],
        compiler_params=params(12),
        cost_estimate=pl.CostEstimate(
            flops=2 * slots * rows * half, bytes_accessed=slots * half * 2, transcendentals=0
        ),
        name="grad",
    )(*[received[d] for d in range(owners)])
    other = lax.ppermute(squares, "width", [(s, halves - 1 - s) for s in range(halves)])
    first, new_moment = pl.pallas_call(
        moment_kernel,
        out_shape=[pltpu.VMEM((rows, half), F32), jax.ShapeDtypeStruct((rows, half), BF16)],
        in_specs=[VMEM] * 3,
        out_specs=[VMEM, ANY],
        scratch_shapes=[pltpu.VMEM((rows, half), BF16), pltpu.SemaphoreType.DMA((rows // LANES,))],
        compiler_params=params(16),
        cost_estimate=pl.CostEstimate(flops=10**9, bytes_accessed=2 * rows * half, transcendentals=0),
        name="moment",
    )(near(grad), near(count), near(moment))
    new_weights, new_scale = pl.pallas_call(
        functools.partial(weights_kernel, halves * half),
        out_shape=[jax.ShapeDtypeStruct((rows, half), BF16), lined],
        in_specs=[VMEM] * 7,
        out_specs=[ANY, VMEM],
        scratch_shapes=[pltpu.VMEM((rows, half), BF16), pltpu.VMEM((rows, LANES), F32), pltpu.SemaphoreType.DMA((rows // LANES,))],
        compiler_params=params(16),
        name="weights",
    )(
        near(first), near(weights), squares, other, hits,
        row_scale.reshape(rows // LANES, LANES), row_steps.reshape(rows // LANES, LANES),
    )
    return new_weights, new_moment, new_scale.reshape(rows)


def solution(mesh):
    return jax.shard_map(
        shards,
        mesh=mesh,
        in_specs=(
            P("vocab", "width"),
            P("vocab"),
            P("vocab", None),
            P("vocab", None),
            P("vocab", "width"),
            P("vocab", "width"),
            P("vocab"),
            P("vocab"),
        ),
        out_specs=(P("vocab", "width"), P("vocab", "width"), P("vocab")),
        check_vma=False,
    )
```

```python
import functools

import jax
import jax.numpy as jnp
from jax import lax
from jax.experimental import pallas as pl
from jax.experimental.pallas import tpu as pltpu
from jax.sharding import PartitionSpec as P


LANES = 128
MIB = 1 << 20
VMEM = pl.BlockSpec(memory_space=pltpu.VMEM)
SMEM = pl.BlockSpec(memory_space=pltpu.SMEM)
ANY = pl.BlockSpec(memory_space=pl.ANY)
F32, BF16, I32 = jnp.float32, jnp.bfloat16, jnp.int32


def iota(shape, axis):
    return lax.broadcasted_iota(I32, shape, axis)


def name_rows(slots):
    return -(-2 * (slots // LANES) // 8) * 8


def col_step(half):
    return 2 * LANES if half % (2 * LANES) == 0 else LANES


def send_kernel(
    owners, cap, me_ref, counts_far, slot_far, rows_far, grads_ref, *rest
):
    outs, rest = rest[:owners], rest[owners:]
    onehot, buf, counts_ref, slot_ref, rows_ref, sems, small = rest
    tokens, half = grads_ref.shape
    slots = owners * cap
    step = col_step(half)
    copies = [
        pltpu.make_async_copy(
            grads_ref.at[:, pl.ds(c, step)], buf.at[:, pl.ds(c, step)], sems.at[c // step]
        )
        for c in range(0, half, step)
    ]
    arrivals = [
        pltpu.make_async_copy(far, ref, small.at[i])
        for i, (far, ref) in enumerate(
            ((slot_far, slot_ref), (rows_far, rows_ref), (counts_far, counts_ref))
        )
    ]
    for copy in arrivals + copies:
        copy.start()
    for copy in arrivals:
        copy.wait()
    me = me_ref[0]
    groups = slots // LANES
    turned = jnp.bitwise_xor(slot_ref[...], me * cap)
    for t in range(tokens // LANES):
        hit = turned[t : t + 1, :] == iota((slots, LANES), 0)
        onehot[:, t * LANES : (t + 1) * LANES] = jnp.where(hit, 1.0, 0.0).astype(BF16)
    lane = iota((1, slots), 1)
    owner, within = lane // cap, lax.rem(lane, cap)
    live = jnp.zeros((1, slots), I32)
    for o in range(owners):
        live = jnp.where((owner == o) & (within < counts_ref[0, o]), 1, live)
    rows = rows_ref[...]
    high = (rows // LANES + 1) * live
    low = lax.rem(rows, LANES) * live
    digits = jnp.concatenate(
        [high.astype(F32), low.astype(F32), jnp.zeros((6, slots), F32)], axis=0
    ).astype(BF16)
    turn = jnp.where(
        iota((slots, slots), 0) == jnp.bitwise_xor(iota((slots, slots), 1), me * cap), 1.0, 0.0
    ).astype(BF16)
    digits = jnp.dot(digits, turn, preferred_element_type=F32)
    pad = name_rows(slots) - 2 * groups
    names = [digits[0:1, g * LANES : (g + 1) * LANES] for g in range(groups)]
    names += [digits[1:2, g * LANES : (g + 1) * LANES] for g in range(groups)]
    if pad:
        names.append(jnp.zeros((pad, LANES), F32))
    names = jnp.concatenate(names, axis=0)
    base = half // LANES * cap
    sub, at = iota(names.shape, 0), iota(names.shape, 1)
    place = (lax.rem(sub, groups) * LANES + at) // cap
    for d in range(owners):
        outs[d][base:, :] = jnp.where(place == d, names, 0.0).astype(BF16)
    for c in range(0, half, step):
        copies[c // step].wait()
        got = jnp.dot(onehot[...], buf[:, c : c + step], preferred_element_type=F32).astype(BF16)
        for d in range(owners):
            for t in range(step // LANES):
                row = (c // LANES + t) * cap
                outs[d][row : row + cap, :] = got[
                    d * cap : (d + 1) * cap, t * LANES : (t + 1) * LANES
                ]


def eye():
    return iota((LANES, LANES), 0) == iota((LANES, LANES), 1)


def to_column(line):
    return jnp.sum(jnp.where(eye(), line, 0.0), axis=1, keepdims=True)


def to_line(column):
    return jnp.sum(jnp.where(eye(), column, 0.0), axis=0, keepdims=True)


def fetch_kernel(
    weights_far, moment_far, scale_ref, steps_ref, weights_ref, moment_ref, rate_ref, fix_ref, row_ref, sems
):
    copies = [
        pltpu.make_async_copy(moment_far, moment_ref, sems.at[0]),
        pltpu.make_async_copy(weights_far, weights_ref, sems.at[1]),
    ]
    for copy in copies:
        copy.start()
    steps = (steps_ref[...] + 1).astype(F32)
    rate = 0.01 / (1.0 - jnp.exp(steps * jnp.log(jnp.float32(0.9))))
    fix = 1.0 / (1.0 - jnp.exp(steps * jnp.log(jnp.float32(0.95))))
    for i in range(steps.shape[0]):
        part = slice(i * LANES, (i + 1) * LANES)
        for line, ref in ((rate, rate_ref), (fix, fix_ref), (scale_ref, row_ref)):
            ref[part, :] = jnp.broadcast_to(to_column(line[i : i + 1, :]), (LANES, LANES))
    for copy in copies:
        copy.wait()


def gather_columns(blocks, cap, c, step):
    parts = []
    for t in range(step // LANES):
        at = (c // LANES + t) * cap
        parts.append(jnp.concatenate([b[at : at + cap, :] for b in blocks], axis=0))
    return jnp.concatenate(parts, axis=1) if len(parts) > 1 else parts[0]


def square_kernel(owners, cap, half, *refs):
    blocks = refs[:owners]
    squares_ref, names_ref, same = refs[owners:]
    slots = owners * cap
    groups = slots // LANES
    step = col_step(half)
    base = half // LANES * cap
    names = blocks[0][base:, :].astype(F32)
    for d in range(1, owners):
        names = names + blocks[d][base:, :].astype(F32)
    row = (names[0:groups, :] - 1.0) * LANES + names[groups : 2 * groups, :]
    names_ref[...] = row.astype(I32)
    for g in range(groups):
        column = to_column(row[g : g + 1, :])
        for h in range(groups):
            hit = column == row[h : h + 1, :]
            same[g * LANES : (g + 1) * LANES, h * LANES : (h + 1) * LANES] = jnp.where(
                hit, 1.0, 0.0
            ).astype(BF16)
    total = None
    for c in range(0, half, step):
        got = jnp.dot(
            same[...], gather_columns(blocks, cap, c, step), preferred_element_type=F32
        )
        for t in range(step // LANES):
            x = got[:, t * LANES : (t + 1) * LANES]
            total = x * x if total is None else total + x * x
    for g in range(groups):
        column = jnp.sum(total[g * LANES : (g + 1) * LANES, :], axis=1, keepdims=True)
        squares_ref[g : g + 1, :] = to_line(column)


def moment_kernel(owners, cap, *refs):
    blocks, names_ref, moment_ref = refs[:owners], refs[owners], refs[owners + 1]
    first_ref, new_ref, place, keep, staged, sems = refs[owners + 2 :]
    rows, half = moment_ref.shape
    slots = owners * cap
    step = col_step(half)
    for g in range(slots // LANES):
        hit = names_ref[g : g + 1, :] == iota((rows, LANES), 0)
        place[:, g * LANES : (g + 1) * LANES] = jnp.where(hit, 1.0, 0.0).astype(BF16)
    count = jnp.dot(place[...], jnp.ones((slots, LANES), BF16), preferred_element_type=F32)
    keep[...] = jnp.where(count > 0.0, 0.9, 1.0)
    copies = []
    block = min(rows, 2 * LANES)
    for c in range(0, half, step):
        got = gather_columns(blocks, cap, c, step)
        for r in range(0, rows, block):
            part = slice(r, r + block)
            grad = jnp.dot(place[part, :], got, preferred_element_type=F32)
            for t in range(step // LANES):
                at = slice(c + t * LANES, c + (t + 1) * LANES)
                first = keep[part, :] * moment_ref[part, at].astype(F32)
                first = first + 0.1 * grad[:, t * LANES : (t + 1) * LANES]
                first_ref[part, at] = first
                staged[part, at] = first.astype(BF16)
        at = pl.ds(c, step)
        copy = pltpu.make_async_copy(staged.at[:, at], new_ref.at[:, at], sems.at[c // step])
        copy.start()
        copies.append(copy)
    for copy in copies:
        copy.wait()


def weights_kernel(
    width, first_ref, weights_ref, mine_ref, other_ref, names_ref, rate_ref, fix_ref, row_ref,
    new_ref, new_scale_ref, staged, rates, sems,
):
    rows, half = first_ref.shape
    groups = names_ref.shape[0]
    square = mine_ref[...] + other_ref[...]
    names = names_ref[...]

    def scalars(i):
        part = slice(i * LANES, (i + 1) * LANES)
        ids = iota((LANES, LANES), 0) + i * LANES
        most = jnp.full((LANES, LANES), -1.0, F32)
        for g in range(groups):
            hit = names[g : g + 1, :] == ids
            most = jnp.maximum(most, jnp.where(hit, square[g : g + 1, :], -1.0))
        most = jnp.broadcast_to(jnp.max(most, axis=1, keepdims=True), (LANES, LANES))
        touched = most >= 0.0
        scale = row_ref[part, :]
        second = jnp.where(touched, 0.95 * scale + 0.05 * (most / width), scale)
        new_scale_ref[i : i + 1, :] = to_line(second)
        denom = jnp.sqrt(second * fix_ref[part, :]) + 1e-08
        rates[part, :] = jnp.where(touched, rate_ref[part, :] / denom, -1.0)

    copies = []
    strip = 16
    for i in range(rows // LANES):
        scalars(i)
    for i in range(rows // LANES):
        for r in range(i * LANES, (i + 1) * LANES, strip):
            part = slice(r, r + strip)
            rate = rates[part, :]
            keep = jnp.where(rate < 0.0, 1.0, 0.999)
            rate = jnp.maximum(rate, 0.0)
            for c in range(0, half, LANES):
                old = weights_ref[part, c : c + LANES].astype(F32)
                new = keep * old - rate * first_ref[part, c : c + LANES]
                staged[part, c : c + LANES] = new.astype(BF16)
        part = pl.ds(i * LANES, LANES)
        copy = pltpu.make_async_copy(staged.at[part, :], new_ref.at[part, :], sems.at[i])
        copy.start()
        copies.append(copy)
    for copy in copies:
        copy.wait()


def near(x):
    return pltpu.with_memory_space_constraint(x, pltpu.VMEM)


def far(x):
    return pltpu.with_memory_space_constraint(x, pltpu.HBM)


def params(limit):
    return pltpu.CompilerParams(vmem_limit_bytes=limit * MIB)


def shards(token_grads, token_slot, slot_rows, counts, weights, moment, row_scale, row_steps):
    owners = lax.axis_size("vocab")
    halves = lax.axis_size("width")
    slots = slot_rows.shape[1]
    cap = slots // owners
    tokens, half = token_grads.shape
    rows = weights.shape[0]
    assert owners & (owners - 1) == 0 and cap & (cap - 1) == 0
    assert rows % LANES == 0 and tokens % LANES == 0 and slots % LANES == 0 and half % LANES == 0
    me = lax.axis_index("vocab").astype(I32).reshape(1)
    height = half // LANES * cap + name_rows(slots)
    step = col_step(half)
    block = jax.ShapeDtypeStruct((height, LANES), BF16)
    outgoing = pl.pallas_call(
        functools.partial(send_kernel, owners, cap),
        out_shape=[block] * owners,
        in_specs=[SMEM, ANY, ANY, ANY, ANY],
        out_specs=[VMEM] * owners,
        scratch_shapes=[
            pltpu.VMEM((slots, tokens), BF16),
            pltpu.VMEM((tokens, half), BF16),
            pltpu.SMEM((1, owners), I32),
            pltpu.VMEM((tokens // LANES, LANES), I32),
            pltpu.VMEM((1, slots), I32),
            pltpu.SemaphoreType.DMA((half // step,)),
            pltpu.SemaphoreType.DMA((3,)),
        ],
        compiler_params=params(24),
        cost_estimate=pl.CostEstimate(
            flops=2 * slots * tokens * half, bytes_accessed=tokens * half * 2, transcendentals=0
        ),
        name="send",
    )(
        me, far(counts), far(token_slot.reshape(tokens // LANES, LANES)), far(slot_rows),
        far(token_grads),
    )
    received = {0: outgoing[0]}
    for d in range(1, owners):
        received[d] = lax.ppermute(outgoing[d], "vocab", [(s, s ^ d) for s in range(owners)])
    lined = jax.ShapeDtypeStruct((rows // LANES, LANES), F32)
    wide = pltpu.VMEM((rows, LANES), F32)
    kept = pltpu.VMEM((rows, half), BF16)
    weights_near, moment_near, rate, fix, scale = pl.pallas_call(
        fetch_kernel,
        out_shape=[kept, kept, wide, wide, wide],
        in_specs=[ANY, ANY, VMEM, VMEM],
        out_specs=[VMEM] * 5,
        scratch_shapes=[pltpu.SemaphoreType.DMA((2,))],
        compiler_params=params(4),
        name="fetch",
    )(
        far(weights), far(moment), row_scale.reshape(rows // LANES, LANES),
        row_steps.reshape(rows // LANES, LANES),
    )
    blocks = [received[d] for d in range(owners)]
    sloted = (slots // LANES, LANES)
    squares, names = pl.pallas_call(
        functools.partial(square_kernel, owners, cap, half),
        out_shape=[jax.ShapeDtypeStruct(sloted, F32), jax.ShapeDtypeStruct(sloted, I32)],
        in_specs=[VMEM] * owners,
        out_specs=[VMEM] * 2,
        scratch_shapes=[pltpu.VMEM((slots, slots), BF16)],
        compiler_params=params(10),
        cost_estimate=pl.CostEstimate(
            flops=2 * slots * slots * half, bytes_accessed=slots * half * 2, transcendentals=0
        ),
        name="square",
    )(*blocks)
    other = lax.ppermute(squares, "width", [(s, halves - 1 - s) for s in range(halves)])
    first, new_moment = pl.pallas_call(
        functools.partial(moment_kernel, owners, cap),
        out_shape=[pltpu.VMEM((rows, half), F32), jax.ShapeDtypeStruct((rows, half), BF16)],
        in_specs=[VMEM] * (owners + 2),
        out_specs=[VMEM, ANY],
        scratch_shapes=[
            pltpu.VMEM((rows, slots), BF16),
            pltpu.VMEM((rows, LANES), F32),
            pltpu.VMEM((rows, half), BF16),
            pltpu.SemaphoreType.DMA((half // step,)),
        ],
        compiler_params=params(16),
        cost_estimate=pl.CostEstimate(
            flops=2 * slots * rows * half, bytes_accessed=2 * rows * half, transcendentals=0
        ),
        name="moment",
    )(*blocks, names, near(moment_near))
    new_weights, new_scale = pl.pallas_call(
        functools.partial(weights_kernel, halves * half),
        out_shape=[jax.ShapeDtypeStruct((rows, half), BF16), lined],
        in_specs=[VMEM] * 8,
        out_specs=[ANY, VMEM],
        scratch_shapes=[
            pltpu.VMEM((rows, half), BF16),
            pltpu.VMEM((rows, LANES), F32),
            pltpu.SemaphoreType.DMA((rows // LANES,)),
        ],
        compiler_params=params(10),
        name="weights",
    )(
        near(first), near(weights_near), squares, other, names, near(rate), near(fix), near(scale),
    )
    return new_weights, new_moment, new_scale.reshape(rows)


def solution(mesh):
    return jax.shard_map(
        shards,
        mesh=mesh,
        in_specs=(
            P("vocab", "width"),
            P("vocab"),
            P("vocab", None),
            P("vocab", None),
            P("vocab", "width"),
            P("vocab", "width"),
            P("vocab"),
            P("vocab"),
        ),
        out_specs=(P("vocab", "width"), P("vocab", "width"), P("vocab")),
        check_vma=False,
    )
```

```python
import functools

import jax
import jax.numpy as jnp
from jax import lax
from jax.experimental import pallas as pl
from jax.experimental.pallas import tpu as pltpu
from jax.sharding import PartitionSpec as P


LANES = 128
MIB = 1 << 20
VMEM = pl.BlockSpec(memory_space=pltpu.VMEM)
SMEM = pl.BlockSpec(memory_space=pltpu.SMEM)
ANY = pl.BlockSpec(memory_space=pl.ANY)
F32, BF16, I32 = jnp.float32, jnp.bfloat16, jnp.int32


REST_FLOPS = 4 * 10**10


def iota(shape, axis):
    return lax.broadcasted_iota(I32, shape, axis)


def name_rows(slots):
    return -(-2 * (slots // LANES) // 8) * 8


def col_step(half):
    return 2 * LANES if half % (2 * LANES) == 0 else LANES


def spread(turned, first, count, onehot):
    for t in range(turned.shape[0]):
        hit = turned[t : t + 1, :] == iota((count, LANES), 0) + first
        onehot[:, t * LANES : (t + 1) * LANES] = jnp.where(hit, 1.0, 0.0).astype(BF16)


def fill(outs, first, cap, slots, half, names, onehot, buf, chunks, ready):
    base = half // LANES * cap
    groups = slots // LANES
    sub, at = iota(names.shape, 0), iota(names.shape, 1)
    place = (lax.rem(sub, groups) * LANES + at) // cap
    for d, out in enumerate(outs):
        out[base:, :] = jnp.where(place == first + d, names, 0.0).astype(BF16)
    for i, (c, step) in enumerate(chunks):
        ready(i)
        got = jnp.dot(onehot[...], buf[:, c : c + step], preferred_element_type=F32).astype(BF16)
        for d, out in enumerate(outs):
            for t in range(step // LANES):
                row = (c // LANES + t) * cap
                out[row : row + cap, :] = got[d * cap : (d + 1) * cap, t * LANES : (t + 1) * LANES]


def chunks_of(half):
    first = (half // LANES + 1) // 2 * LANES
    return (0, first), (first, half - first)


def far_kernel(
    owners, cap, me_ref, counts_far, slot_far, rows_far, grads_far, *rest
):
    outs, rest = rest[: owners // 2], rest[owners // 2 :]
    grads_ref, turned_ref, names_ref, onehot, counts_ref, slot_ref, rows_ref, sems, small = rest
    _, half = grads_ref.shape
    slots = owners * cap
    chunks = chunks_of(half)
    copies = [
        pltpu.make_async_copy(
            grads_far.at[:, pl.ds(c, step)], grads_ref.at[:, pl.ds(c, step)], sems.at[i]
        )
        for i, (c, step) in enumerate(chunks)
    ]
    arrivals = [
        pltpu.make_async_copy(far, ref, small.at[i])
        for i, (far, ref) in enumerate(
            ((slot_far, slot_ref), (rows_far, rows_ref), (counts_far, counts_ref))
        )
    ]
    for copy in arrivals + copies:
        copy.start()
    for copy in arrivals:
        copy.wait()
    me = me_ref[0]
    groups = slots // LANES
    turned = jnp.bitwise_xor(slot_ref[...], me * cap)
    turned_ref[...] = turned
    spread(turned, slots // 2, slots // 2, onehot)
    lane = iota((1, slots), 1)
    owner, within = lane // cap, lax.rem(lane, cap)
    live = jnp.zeros((1, slots), I32)
    for o in range(owners):
        live = jnp.where((owner == o) & (within < counts_ref[0, o]), 1, live)
    rows = rows_ref[...]
    high = (rows // LANES + 1) * live
    low = lax.rem(rows, LANES) * live
    digits = jnp.concatenate(
        [high.astype(F32), low.astype(F32), jnp.zeros((6, slots), F32)], axis=0
    ).astype(BF16)
    turn = jnp.where(
        iota((slots, slots), 0) == jnp.bitwise_xor(iota((slots, slots), 1), me * cap), 1.0, 0.0
    ).astype(BF16)
    digits = jnp.dot(digits, turn, preferred_element_type=F32)
    pad = name_rows(slots) - 2 * groups
    names = [digits[0:1, g * LANES : (g + 1) * LANES] for g in range(groups)]
    names += [digits[1:2, g * LANES : (g + 1) * LANES] for g in range(groups)]
    if pad:
        names.append(jnp.zeros((pad, LANES), F32))
    names = jnp.concatenate(names, axis=0)
    names_ref[...] = names
    fill(
        outs, owners // 2, cap, slots, half, names, onehot, grads_ref, chunks,
        lambda i: copies[i].wait(),
    )


def rest_kernel(owners, cap, turned_ref, names_ref, grads_ref, steps_ref, *rest):
    outs, (rate_ref, fix_ref, onehot) = rest[: owners // 2], rest[owners // 2 :]
    steps = (steps_ref[...] + 1).astype(F32)
    rate = 0.01 / (1.0 - jnp.exp(steps * jnp.log(jnp.float32(0.9))))
    fix = 1.0 / (1.0 - jnp.exp(steps * jnp.log(jnp.float32(0.95))))
    rate_ref[...] = rate
    fix_ref[...] = fix
    half = grads_ref.shape[1]
    slots = owners * cap
    spread(turned_ref[...], 0, slots // 2, onehot)
    fill(
        outs, 0, cap, slots, half, names_ref[...], onehot, grads_ref, chunks_of(half),
        lambda i: None,
    )


def eye():
    return iota((LANES, LANES), 0) == iota((LANES, LANES), 1)


def to_column(line):
    return jnp.sum(jnp.where(eye(), line, 0.0), axis=1, keepdims=True)


def to_line(column):
    return jnp.sum(jnp.where(eye(), column, 0.0), axis=0, keepdims=True)


def gather_columns(blocks, cap, c, step):
    parts = []
    for t in range(step // LANES):
        at = (c // LANES + t) * cap
        parts.append(jnp.concatenate([b[at : at + cap, :] for b in blocks], axis=0))
    return jnp.concatenate(parts, axis=1) if len(parts) > 1 else parts[0]


def square_kernel(owners, cap, half, *refs):
    blocks = refs[:owners]
    squares_ref, names_ref, columns_ref, same = refs[owners:]
    slots = owners * cap
    groups = slots // LANES
    step = col_step(half)
    base = half // LANES * cap
    names = blocks[0][base:, :].astype(F32)
    for d in range(1, owners):
        names = names + blocks[d][base:, :].astype(F32)
    row = (names[0:groups, :] - 1.0) * LANES + names[groups : 2 * groups, :]
    names_ref[...] = row.astype(I32)
    for g in range(groups):
        column = jnp.broadcast_to(to_column(row[g : g + 1, :]), (LANES, LANES))
        columns_ref[g * LANES : (g + 1) * LANES, :] = column
        for h in range(groups):
            hit = column == row[h : h + 1, :]
            same[g * LANES : (g + 1) * LANES, h * LANES : (h + 1) * LANES] = jnp.where(
                hit, 1.0, 0.0
            ).astype(BF16)
    total = None
    for c in range(0, half, step):
        got = jnp.dot(
            same[...], gather_columns(blocks, cap, c, step), preferred_element_type=F32
        )
        for t in range(step // LANES):
            x = got[:, t * LANES : (t + 1) * LANES]
            total = x * x if total is None else total + x * x
    for g in range(groups):
        column = jnp.sum(total[g * LANES : (g + 1) * LANES, :], axis=1, keepdims=True)
        squares_ref[g : g + 1, :] = to_line(column)


def moment_kernel(owners, cap, *refs):
    blocks, names_ref, moment_ref = refs[:owners], refs[owners], refs[owners + 1]
    first_ref, new_ref, touched_ref, place, keep, staged, sems = refs[owners + 2 :]
    rows, half = moment_ref.shape
    slots = owners * cap
    step = col_step(half)
    for g in range(slots // LANES):
        hit = names_ref[g : g + 1, :] == iota((rows, LANES), 0)
        place[:, g * LANES : (g + 1) * LANES] = jnp.where(hit, 1.0, 0.0).astype(BF16)
    count = jnp.dot(place[...], jnp.ones((slots, LANES), BF16), preferred_element_type=F32)
    keep[...] = jnp.where(count > 0.0, 0.9, 1.0)
    touched_ref[...] = count.astype(BF16)
    copies = []
    block = min(rows, 2 * LANES)
    for c in range(0, half, step):
        got = gather_columns(blocks, cap, c, step)
        for r in range(0, rows, block):
            part = slice(r, r + block)
            grad = jnp.dot(place[part, :], got, preferred_element_type=F32)
            for t in range(step // LANES):
                at = slice(c + t * LANES, c + (t + 1) * LANES)
                first = keep[part, :] * moment_ref[part, at].astype(F32)
                first = first + 0.1 * grad[:, t * LANES : (t + 1) * LANES]
                first_ref[part, at] = first
                staged[part, at] = first.astype(BF16)
        at = pl.ds(c, step)
        copy = pltpu.make_async_copy(staged.at[:, at], new_ref.at[:, at], sems.at[c // step])
        copy.start()
        copies.append(copy)
    for copy in copies:
        copy.wait()


def ready_kernel(weights_ref, kept_ref):
    rows, half = weights_ref.shape
    strip = 16

    @pl.loop(0, rows // strip)
    def _(i):
        part = pl.ds(pl.multiple_of(i * strip, strip), strip)
        for c in range(0, half, LANES):
            at = slice(c, c + LANES)
            kept_ref[part, at] = 0.999 * weights_ref[part, at].astype(F32)


def weights_kernel(
    width, first_ref, weights_ref, kept_ref, touched_ref, mine_ref, other_ref, columns_ref,
    rate_ref, fix_ref, scale_ref, new_ref, new_scale_ref, staged, rates, sems,
):
    rows, half = first_ref.shape
    slots = columns_ref.shape[0]
    lines = rows // LANES
    square = mine_ref[...] + other_ref[...]
    most = [jnp.full((LANES, LANES), -1.0, F32)] * lines
    for g in range(slots // LANES):
        column = jnp.broadcast_to(to_column(square[g : g + 1, :]), (LANES, LANES))
        named = columns_ref[g * LANES : (g + 1) * LANES, :]
        for i in range(lines):
            hit = named == (iota((LANES, LANES), 1) + i * LANES).astype(F32)
            most[i] = jnp.maximum(most[i], jnp.where(hit, column, -1.0))
    most = jnp.concatenate([jnp.max(x, axis=0, keepdims=True) for x in most], axis=0)
    scale = scale_ref[...]
    second = jnp.where(most >= 0.0, 0.95 * scale + 0.05 * (most / width), scale)
    new_scale_ref[...] = second
    rate = rate_ref[...] / (jnp.sqrt(second * fix_ref[...]) + 1e-08)
    for i in range(lines):
        column = to_column(rate[i : i + 1, :])
        rates[i * LANES : (i + 1) * LANES, :] = jnp.broadcast_to(column, (LANES, LANES))
    copies = []
    strip = 16
    for i in range(lines):
        for r in range(i * LANES, (i + 1) * LANES, strip):
            part = slice(r, r + strip)
            rate = rates[part, :]
            touched = touched_ref[part, :] > 0
            for c in range(0, half, LANES):
                at = slice(c, c + LANES)
                new = (kept_ref[part, at] - rate * first_ref[part, at]).astype(BF16)
                staged[part, at] = jnp.where(touched, new, weights_ref[part, at])
        part = pl.ds(i * LANES, LANES)
        copy = pltpu.make_async_copy(staged.at[part, :], new_ref.at[part, :], sems.at[i])
        copy.start()
        copies.append(copy)
    for copy in copies:
        copy.wait()


def near(x):
    return pltpu.with_memory_space_constraint(x, pltpu.VMEM)


def far(x):
    return pltpu.with_memory_space_constraint(x, pltpu.HBM)


def params(limit):
    return pltpu.CompilerParams(vmem_limit_bytes=limit * MIB)


def shards(token_grads, token_slot, slot_rows, counts, weights, moment, row_scale, row_steps):
    owners = lax.axis_size("vocab")
    halves = lax.axis_size("width")
    slots = slot_rows.shape[1]
    cap = slots // owners
    tokens, half = token_grads.shape
    rows = weights.shape[0]
    assert owners & (owners - 1) == 0 and cap & (cap - 1) == 0
    assert rows % LANES == 0 and tokens % LANES == 0 and slots % LANES == 0 and half % LANES == 0
    me = lax.axis_index("vocab").astype(I32).reshape(1)
    height = half // LANES * cap + name_rows(slots)
    step = col_step(half)
    block = jax.ShapeDtypeStruct((height, LANES), BF16)
    cost = pl.CostEstimate(
        flops=slots * tokens * half, bytes_accessed=tokens * half * 2, transcendentals=0
    )
    *upper, grads_near, turned, digits = pl.pallas_call(
        functools.partial(far_kernel, owners, cap),
        out_shape=[block] * (owners // 2)
        + [
            pltpu.VMEM((tokens, half), BF16),
            pltpu.VMEM((tokens // LANES, LANES), I32),
            pltpu.VMEM((name_rows(slots), LANES), F32),
        ],
        in_specs=[SMEM, ANY, ANY, ANY, ANY],
        out_specs=[VMEM] * (owners // 2 + 3),
        scratch_shapes=[
            pltpu.VMEM((slots // 2, tokens), BF16),
            pltpu.SMEM((1, owners), I32),
            pltpu.VMEM((tokens // LANES, LANES), I32),
            pltpu.VMEM((1, slots), I32),
            pltpu.SemaphoreType.DMA((2,)),
            pltpu.SemaphoreType.DMA((3,)),
        ],
        compiler_params=params(12),
        cost_estimate=cost,
        name="far",
    )(
        me, far(counts), far(token_slot.reshape(tokens // LANES, LANES)), far(slot_rows),
        far(token_grads),
    )
    lined = jax.ShapeDtypeStruct((rows // LANES, LANES), F32)
    *lower, rate, fix = pl.pallas_call(
        functools.partial(rest_kernel, owners, cap),
        out_shape=[block] * (owners // 2) + [lined] * 2,
        in_specs=[VMEM] * 4,
        out_specs=[VMEM] * (owners // 2 + 2),
        scratch_shapes=[pltpu.VMEM((slots // 2, tokens), BF16)],
        compiler_params=params(12),
        cost_estimate=pl.CostEstimate(flops=REST_FLOPS, bytes_accessed=0, transcendentals=0),
        name="rest",
    )(
        near(turned), near(digits), near(grads_near), row_steps.reshape(rows // LANES, LANES),
    )
    outgoing = list(lower) + list(upper)
    received = {0: outgoing[0]}
    for d in range(1, owners):
        received[d] = lax.ppermute(outgoing[d], "vocab", [(s, s ^ d) for s in range(owners)])
    blocks = [received[d] for d in range(owners)]
    sloted = (slots // LANES, LANES)
    squares, names, name_columns = pl.pallas_call(
        functools.partial(square_kernel, owners, cap, half),
        out_shape=[
            jax.ShapeDtypeStruct(sloted, F32),
            jax.ShapeDtypeStruct(sloted, I32),
            pltpu.VMEM((slots, LANES), F32),
        ],
        in_specs=[VMEM] * owners,
        out_specs=[VMEM] * 3,
        scratch_shapes=[pltpu.VMEM((slots, slots), BF16)],
        compiler_params=params(10),
        cost_estimate=pl.CostEstimate(
            flops=2 * slots * slots * half, bytes_accessed=slots * half * 2, transcendentals=0
        ),
        name="square",
    )(*blocks)
    other = lax.ppermute(squares, "width", [(s, halves - 1 - s) for s in range(halves)])
    kept = pl.pallas_call(
        ready_kernel,
        out_shape=pltpu.VMEM((rows, half), F32),
        in_specs=[VMEM],
        out_specs=VMEM,
        compiler_params=params(2),
        cost_estimate=pl.CostEstimate(flops=2 * rows * half, bytes_accessed=0, transcendentals=0),
        name="ready",
    )(near(weights))
    first, new_moment, touched = pl.pallas_call(
        functools.partial(moment_kernel, owners, cap),
        out_shape=[
            pltpu.VMEM((rows, half), F32),
            jax.ShapeDtypeStruct((rows, half), BF16),
            pltpu.VMEM((rows, LANES), BF16),
        ],
        in_specs=[VMEM] * (owners + 2),
        out_specs=[VMEM, ANY, VMEM],
        scratch_shapes=[
            pltpu.VMEM((rows, slots), BF16),
            pltpu.VMEM((rows, LANES), F32),
            pltpu.VMEM((rows, half), BF16),
            pltpu.SemaphoreType.DMA((half // step,)),
        ],
        compiler_params=params(16),
        cost_estimate=pl.CostEstimate(
            flops=2 * slots * rows * half, bytes_accessed=2 * rows * half, transcendentals=0
        ),
        name="moment",
    )(*blocks, names, near(moment))
    new_weights, new_scale = pl.pallas_call(
        functools.partial(weights_kernel, halves * half),
        out_shape=[jax.ShapeDtypeStruct((rows, half), BF16), lined],
        in_specs=[VMEM] * 10,
        out_specs=[ANY, VMEM],
        scratch_shapes=[
            pltpu.VMEM((rows, half), BF16),
            pltpu.VMEM((rows, LANES), F32),
            pltpu.SemaphoreType.DMA((rows // LANES,)),
        ],
        compiler_params=params(10),
        name="weights",
    )(
        near(first), near(weights), near(kept), near(touched), squares, other, near(name_columns),
        rate, fix, row_scale.reshape(rows // LANES, LANES),
    )
    return new_weights, new_moment, new_scale.reshape(rows)


def solution(mesh):
    return jax.shard_map(
        shards,
        mesh=mesh,
        in_specs=(
            P("vocab", "width"),
            P("vocab"),
            P("vocab", None),
            P("vocab", None),
            P("vocab", "width"),
            P("vocab", "width"),
            P("vocab"),
            P("vocab"),
        ),
        out_specs=(P("vocab", "width"), P("vocab", "width"), P("vocab")),
        check_vma=False,
    )
```
